32 devices in a mesh: band: 4 (over y, core), grid: 8 (over z, x).
Axes of the slice: x: 2, y: 2, z: 4, core: 2. Of those that a mesh axis runs over, the one named last changes fastest.
Arguments:
- orbitals: bfloat16 [64, 2, 16, 128, 128], P('band', None, 'grid'), may hold values from -1.5 to 1.5
- occupations: float32 [64], P('band'), may hold values from 0.2 to 2
Outputs:
- current: float32 [3, 16, 128, 128], P(None, 'grid', 'band')
The draws below stay inside these ranges and needn't reach their ends.
All inputs are finite; a program needn't handle non-finite values.
Results may differ from the reference program's by a relative error of at most 0.0003.
Values may be sent and summed in bfloat16 or wider, within the bound.
A program may use at most 64 MiB of HBM per device.

```python
import jax
import jax.numpy as jnp
from jax import lax

NX = 128
NY = 128
BANDS = 64
NZ = 16


def block_scale(key, extent, cuts, smallest, top_value):
    def one(axis_at, parts):
        steps = jax.random.uniform(jax.random.fold_in(jax.random.fold_in(key, 6), axis_at), (parts,), jnp.float32, smallest / len(cuts), top_value / len(cuts))
        return jnp.repeat(jnp.exp(steps), extent[axis_at] // parts).reshape((-1,) + (1,) * (len(extent) - axis_at - 1))

    level = one(*cuts[0])
    for cut in cuts[1:]:
        level = level * one(*cut)
    return level


def normal_values(key, shape, width, reach, pieces=(), held_as=jnp.bfloat16):
    entries = width * jax.random.normal(key, shape, jnp.float32)
    if pieces:
        entries = entries * block_scale(key, shape, pieces, -0.22, 0.18)
    return jnp.clip(entries, -reach, reach).astype(held_as)


def setup_inputs(seed: int = 0) -> dict:
    splits = jax.random.split(jax.random.key(seed), 3)
    return {
        "orbitals": normal_values(splits[0], (BANDS, 2, NZ, NX, NY), 0.25, 1.5, ((0, 4), (2, 8))),
        "occupations": jnp.clip(0.2 + 1.8 * jax.random.uniform(splits[1], (BANDS,), jnp.float32) ** block_scale(splits[1], (BANDS,), ((0, 4),), -0.2, 0.2), 0.2, 2.0),
    }


def derivative(values, direction):
    forward = jnp.roll(values, -1, direction) - jnp.roll(values, 1, direction)
    farther = jnp.roll(values, -2, direction) - jnp.roll(values, 2, direction)
    return (8.0 * forward - farther) / 12.0


def reference(orbitals, occupations):
    def advance(summed, item):
        orbital, weight = item
        real_part = orbital[0].astype(jnp.float32)
        imag_part = orbital[1].astype(jnp.float32)
        components = jnp.stack([real_part * derivative(imag_part, direction) - imag_part * derivative(real_part, direction) for direction in range(3)])
        return summed + weight * components, None

    initial = jnp.zeros((3, NZ, NX, NY), jnp.float32)
    summed, _ = lax.scan(advance, initial, (orbitals, occupations))
    return summed
```

```python
import functools

import jax
import jax.numpy as jnp
from jax import lax
from jax.experimental import pallas as pl
from jax.experimental.pallas import tpu as pltpu
from jax.sharding import PartitionSpec as P

CHUNK = 16


def stencil(n, flipped):
    row = lax.broadcasted_iota(jnp.int32, (n, n), 0)
    col = lax.broadcasted_iota(jnp.int32, (n, n), 1)
    d = col - row if flipped else row - col
    value = jnp.zeros((n, n), jnp.float32)
    for step, weight in ((1, 8.0), (-1, -8.0), (2, -1.0), (-2, 1.0)):
        hit = (d == step) | (d == step - n) | (d == step + n)
        value = jnp.where(hit, weight, value)
    return value.astype(jnp.bfloat16)


def kernel(
    nb, ng, occ_ref, orb_ref, out_ref,
    own, mate, outer, mx, my, plane_sum, plane_recv, zsend, zrecv,
    own_sem, mate_send, mate_recv, outer_send, outer_recv,
    plane_send_sem, plane_recv_sem, z_send_sem, z_recv_sem,
):
    bands, _, depth, nx, ny = orb_ref.shape
    b = lax.axis_index("band")
    g = lax.axis_index("grid")
    odd = lax.rem(g, 2)
    turn = 1 - 2 * odd
    partner = g + turn
    ahead = lax.rem(g + 2 * turn + ng, ng)
    behind = lax.rem(g - 2 * turn + ng, ng)
    rows = nx // nb
    subs = rows // CHUNK
    chunks = (nb // 2) * subs

    load = pltpu.make_async_copy(orb_ref, own, own_sem)
    load.start()

    barrier = pltpu.get_barrier_semaphore()
    count = 0
    for k in range(nb):
        peer = lax.rem(b + k, nb)
        for at in (g, partner, ahead, behind):
            if k == 0 and at is g:
                continue
            pl.semaphore_signal(barrier, inc=1, device_id={"band": peer, "grid": at})
            count += 1
    pl.semaphore_wait(barrier, count)

    def start_of(chunk, parity):
        block = (chunk // subs) * 2 + parity
        return pl.multiple_of(block * rows + (chunk % subs) * CHUNK, CHUNK)

    def to_mate(c):
        return pltpu.make_async_remote_copy(
            src_ref=orb_ref.at[:, :, :, pl.ds(start_of(c, 1 - odd), CHUNK), :],
            dst_ref=mate.at[c],
            send_sem=mate_send.at[c],
            recv_sem=mate_recv.at[c],
            device_id={"band": b, "grid": partner},
        )

    def to_outer(c):
        return pltpu.make_async_remote_copy(
            src_ref=orb_ref.at[:, :, :, pl.ds(start_of(c, odd), CHUNK), :],
            dst_ref=outer.at[c],
            send_sem=outer_send.at[c],
            recv_sem=outer_recv.at[c],
            device_id={"band": b, "grid": behind},
        )

    for c in range(chunks):
        to_mate(c).start()
        to_outer(c).start()

    mx[...] = stencil(nx, True)
    my[...] = stencil(ny, False)
    plane_sum[...] = jnp.zeros_like(plane_sum)
    load.wait()

    def lateral(n, carry):
        w = occ_ref[n]
        for s in range(depth):
            re = own[n, 0, s]
            im = own[n, 1, s]
            tx = jnp.dot(mx[...], jnp.concatenate([re, im], 1), preferred_element_type=jnp.float32)
            ty = jnp.dot(jnp.concatenate([re, im], 0), my[...], preferred_element_type=jnp.float32)
            wre = re.astype(jnp.float32) * w
            wim = im.astype(jnp.float32) * w
            plane_sum[0, s] += wre * tx[:, ny:] - wim * tx[:, :ny]
            plane_sum[1, s] += wre * ty[nx:] - wim * ty[:nx]
        return carry

    lax.fori_loop(0, bands, lateral, 0)

    def to_peer(k):
        peer = lax.rem(b + k, nb)
        return pltpu.make_async_remote_copy(
            src_ref=plane_sum.at[:, :, pl.ds(pl.multiple_of(peer * rows, rows), rows), :],
            dst_ref=plane_recv.at[k - 1],
            send_sem=plane_send_sem.at[k - 1],
            recv_sem=plane_recv_sem.at[k - 1],
            device_id={"band": peer, "grid": g},
        )

    for k in range(1, nb):
        to_peer(k).start()

    sign = turn.astype(jnp.float32)
    first = odd
    second = 1 - odd

    def to_owner(c, slab):
        at = (g, partner, ahead)[slab]
        sub = c % subs
        return pltpu.make_async_remote_copy(
            src_ref=zsend.at[c, slab],
            dst_ref=zrecv.at[slab // 2, b, :, pl.ds(sub * CHUNK, CHUNK), :],
            send_sem=z_send_sem.at[c, slab],
            recv_sem=z_recv_sem.at[slab // 2, b, sub],
            device_id={"band": (c // subs) * 2 + odd, "grid": at},
        )

    for c in range(chunks):
        start = start_of(c, odd)
        to_mate(c).wait_recv()
        to_outer(c).wait_recv()

        def depthwise(n, sums):
            w = occ_ref[n] * sign
            fields = []
            for p in (first, second):
                fields.append(tuple(own[n, q, p, pl.ds(start, CHUNK), :].astype(jnp.float32) for q in (0, 1)))
            for held in (mate, outer):
                for p in (first, second):
                    fields.append(tuple(held[c, n, q, p].astype(jnp.float32) for q in (0, 1)))
            scaled = [(re * w, im * w) for re, im in fields[:4]]
            pairs = ((0, 1), (1, 2), (2, 3), (3, 4), (0, 2), (1, 3), (2, 4), (3, 5))
            return tuple(
                total + (scaled[i][0] * fields[j][1] - scaled[i][1] * fields[j][0])
                for total, (i, j) in zip(sums, pairs)
            )

        zero = jnp.zeros((CHUNK, ny), jnp.float32)
        n01, n12, n23, n34, f02, f13, f24, f35 = lax.fori_loop(0, bands, depthwise, (zero,) * 8)
        parts = (
            (8.0 * n01 - f02, 8.0 * (n01 + n12) - f13),
            (8.0 * (n12 + n23) - f02 - f24, 8.0 * (n23 + n34) - f13 - f35),
            (8.0 * n34 - f24, -f35),
        )
        owner = (c // subs) * 2 + odd
        for slab in (1, 2, 0):
            zsend[c, slab, first] = parts[slab][0]
            zsend[c, slab, second] = parts[slab][1]
            if slab:
                to_owner(c, slab).start()
            else:
                @pl.when(owner != b)
                def _():
                    to_owner(c, 0).start()

                @pl.when(owner == b)
                def _():
                    here = pl.ds((c % subs) * CHUNK, CHUNK)
                    zrecv[0, b, first, here, :] = parts[0][0]
                    zrecv[0, b, second, here, :] = parts[0][1]

    mine = pl.ds(pl.multiple_of(b * rows, rows), rows)
    summed = plane_sum[:, :, mine, :]
    for k in range(1, nb):
        to_peer(k).wait_recv()
        summed = summed + plane_recv[k - 1]
    out_ref[1:3] = summed * (1.0 / 12.0)

    def arrival(kind, source):
        for sub in range(subs):
            pltpu.make_async_remote_copy(
                src_ref=zsend.at[0, 0],
                dst_ref=zrecv.at[kind, source, :, pl.ds(sub * CHUNK, CHUNK), :],
                send_sem=z_send_sem.at[0, 0],
                recv_sem=z_recv_sem.at[kind, source, sub],
                device_id={"band": b, "grid": partner},
            ).wait_recv()

    alike = lax.rem(b, 2) == odd

    @pl.when(alike)
    def _():
        for source in range(nb):
            @pl.when(b != source)
            def _():
                arrival(0, source)
        for source in range(nb):
            arrival(1, source)
        out_ref[0] = (jnp.sum(zrecv[0], 0) + jnp.sum(zrecv[1], 0)) * (1.0 / 12.0)

    @pl.when(jnp.logical_not(alike))
    def _():
        for source in range(nb):
            arrival(0, source)
        out_ref[0] = jnp.sum(zrecv[0], 0) * (1.0 / 12.0)

    for k in range(1, nb):
        to_peer(k).wait_send()
    for c in range(chunks):
        to_mate(c).wait_send()
        to_outer(c).wait_send()
        to_owner(c, 1).wait_send()
        to_owner(c, 2).wait_send()

        @pl.when((c // subs) * 2 + odd != b)
        def _():
            to_owner(c, 0).wait_send()


def solution(mesh):
    nb = mesh.shape["band"]
    ng = mesh.shape["grid"]

    def per_device(orbitals, occupations):
        bands, _, depth, nx, ny = orbitals.shape
        rows = nx // nb
        if depth != 2 or nb % 2 or ng % 2 or ng < 4 or rows % CHUNK:
            raise ValueError("unsupported sizes")
        subs = rows // CHUNK
        chunks = (nb // 2) * subs
        f32, bf16 = jnp.float32, jnp.bfloat16
        dma = pltpu.SemaphoreType.DMA
        return pl.pallas_call(
            functools.partial(kernel, nb, ng),
            out_shape=jax.ShapeDtypeStruct((3, depth, rows, ny), f32),
            in_specs=[
                pl.BlockSpec(memory_space=pltpu.SMEM),
                pl.BlockSpec(memory_space=pl.ANY),
            ],
            out_specs=pl.BlockSpec(memory_space=pltpu.VMEM),
            scratch_shapes=[
                pltpu.VMEM((bands, 2, depth, nx, ny), bf16),
                pltpu.VMEM((chunks, bands, 2, depth, CHUNK, ny), bf16),
                pltpu.VMEM((chunks, bands, 2, depth, CHUNK, ny), bf16),
                pltpu.VMEM((nx, nx), bf16),
                pltpu.VMEM((ny, ny), bf16),
                pltpu.VMEM((2, depth, nx, ny), f32),
                pltpu.VMEM((nb - 1, 2, depth, rows, ny), f32),
                pltpu.VMEM((chunks, 3, depth, CHUNK, ny), f32),
                pltpu.VMEM((2, nb, depth, rows, ny), f32),
                dma,
                dma((chunks,)),
                dma((chunks,)),
                dma((chunks,)),
                dma((chunks,)),
                dma((nb - 1,)),
                dma((nb - 1,)),
                dma((chunks, 3)),
                dma((2, nb, subs)),
            ],
            compiler_params=pltpu.CompilerParams(collective_id=0, has_side_effects=True),
            name="current",
        )(occupations, orbitals)

    return jax.shard_map(
        per_device,
        mesh=mesh,
        in_specs=(P("band", None, "grid", None, None), P("band")),
        out_specs=P(None, "grid", "band", None),
        check_vma=False,
    )
```

```python
import functools

import jax
import jax.numpy as jnp
from jax import lax
from jax.experimental import pallas as pl
from jax.experimental.pallas import tpu as pltpu
from jax.sharding import PartitionSpec as P

CHUNK = 16


def stencil(n, flipped):
    row = lax.broadcasted_iota(jnp.int32, (n, n), 0)
    col = lax.broadcasted_iota(jnp.int32, (n, n), 1)
    d = col - row if flipped else row - col
    value = jnp.zeros((n, n), jnp.float32)
    for step, weight in ((1, 8.0), (-1, -8.0), (2, -1.0), (-2, 1.0)):
        hit = (d == step) | (d == step - n) | (d == step + n)
        value = jnp.where(hit, weight, value)
    return value.astype(jnp.bfloat16)


def kernel(
    nb, ng, occ_ref, orb_ref, out_ref,
    own, mate, outer, mx, my, plane_sum, plane_recv, zsend, zrecv,
    own_sem, mate_send, mate_recv, outer_send, outer_recv,
    plane_send_sem, plane_recv_sem, z_send_sem, z_recv_sem, ready,
):
    bands, _, depth, nx, ny = orb_ref.shape
    b = lax.axis_index("band")
    g = lax.axis_index("grid")
    odd = lax.rem(g, 2)
    turn = 1 - 2 * odd
    partner = g + turn
    ahead = lax.rem(g + 2 * turn + ng, ng)
    behind = lax.rem(g - 2 * turn + ng, ng)
    rows = nx // nb
    subs = rows // CHUNK
    chunks = (nb // 2) * subs

    load = pltpu.make_async_copy(orb_ref, own, own_sem)
    load.start()

    barrier = pltpu.get_barrier_semaphore()
    peers = [lax.rem(b + k, nb) for k in range(1, nb)]
    direct = [(b, partner), (b, ahead), (b, behind)] + [(peer, g) for peer in peers]
    for band, grid in direct:
        pl.semaphore_signal(barrier, inc=1, device_id={"band": band, "grid": grid})
    pl.semaphore_wait(barrier, len(direct))

    def start_of(chunk, parity):
        block = (chunk // subs) * 2 + parity
        return pl.multiple_of(block * rows + (chunk % subs) * CHUNK, CHUNK)

    def to_mate(c):
        return pltpu.make_async_remote_copy(
            src_ref=orb_ref.at[:, :, :, pl.ds(start_of(c, 1 - odd), CHUNK), :],
            dst_ref=mate.at[c],
            send_sem=mate_send.at[c],
            recv_sem=mate_recv.at[c],
            device_id={"band": b, "grid": partner},
        )

    def to_outer(c):
        return pltpu.make_async_remote_copy(
            src_ref=orb_ref.at[:, :, :, pl.ds(start_of(c, odd), CHUNK), :],
            dst_ref=outer.at[c],
            send_sem=outer_send.at[c],
            recv_sem=outer_recv.at[c],
            device_id={"band": b, "grid": behind},
        )

    for c in range(chunks):
        to_mate(c).start()
        to_outer(c).start()
    for peer in peers:
        pl.semaphore_signal(ready, inc=1, device_id={"band": peer, "grid": g})

    mx[...] = stencil(nx, True)
    my[...] = stencil(ny, False)
    plane_sum[...] = jnp.zeros_like(plane_sum)
    load.wait()

    def lateral(n, carry):
        w = occ_ref[n]
        for s in range(depth):
            re = own[n, 0, s]
            im = own[n, 1, s]
            tx = jnp.dot(mx[...], jnp.concatenate([re, im], 1), preferred_element_type=jnp.float32)
            ty = jnp.dot(jnp.concatenate([re, im], 0), my[...], preferred_element_type=jnp.float32)
            wre = re.astype(jnp.float32) * w
            wim = im.astype(jnp.float32) * w
            plane_sum[0, s] += wre * tx[:, ny:] - wim * tx[:, :ny]
            plane_sum[1, s] += wre * ty[nx:] - wim * ty[:nx]
        return carry

    lax.fori_loop(0, bands, lateral, 0)

    def to_peer(k):
        peer = lax.rem(b + k, nb)
        return pltpu.make_async_remote_copy(
            src_ref=plane_sum.at[:, :, pl.ds(pl.multiple_of(peer * rows, rows), rows), :],
            dst_ref=plane_recv.at[k - 1],
            send_sem=plane_send_sem.at[k - 1],
            recv_sem=plane_recv_sem.at[k - 1],
            device_id={"band": peer, "grid": g},
        )

    for k in range(1, nb):
        to_peer(k).start()

    pl.semaphore_wait(ready, nb - 1)
    sign = turn.astype(jnp.float32)
    first = odd
    second = 1 - odd

    def to_owner(c, slab):
        at = (g, partner, ahead)[slab]
        sub = c % subs
        return pltpu.make_async_remote_copy(
            src_ref=zsend.at[c, slab],
            dst_ref=zrecv.at[slab // 2, b, :, pl.ds(sub * CHUNK, CHUNK), :],
            send_sem=z_send_sem.at[c, slab],
            recv_sem=z_recv_sem.at[slab // 2, b, sub],
            device_id={"band": (c // subs) * 2 + odd, "grid": at},
        )

    for c in range(chunks):
        start = start_of(c, odd)
        to_mate(c).wait_recv()
        to_outer(c).wait_recv()

        def depthwise(n, sums):
            w = occ_ref[n] * sign
            fields = []
            for p in (first, second):
                fields.append(tuple(own[n, q, p, pl.ds(start, CHUNK), :].astype(jnp.float32) for q in (0, 1)))
            for held in (mate, outer):
                for p in (first, second):
                    fields.append(tuple(held[c, n, q, p].astype(jnp.float32) for q in (0, 1)))
            scaled = [(re * w, im * w) for re, im in fields[:4]]
            pairs = ((0, 1), (1, 2), (2, 3), (3, 4), (0, 2), (1, 3), (2, 4), (3, 5))
            return tuple(
                total + (scaled[i][0] * fields[j][1] - scaled[i][1] * fields[j][0])
                for total, (i, j) in zip(sums, pairs)
            )

        zero = jnp.zeros((CHUNK, ny), jnp.float32)
        n01, n12, n23, n34, f02, f13, f24, f35 = lax.fori_loop(0, bands, depthwise, (zero,) * 8)
        parts = (
            (8.0 * n01 - f02, 8.0 * (n01 + n12) - f13),
            (8.0 * (n12 + n23) - f02 - f24, 8.0 * (n23 + n34) - f13 - f35),
            (8.0 * n34 - f24, -f35),
        )
        owner = (c // subs) * 2 + odd
        for slab in (1, 2, 0):
            zsend[c, slab, first] = parts[slab][0]
            zsend[c, slab, second] = parts[slab][1]
            if slab:
                to_owner(c, slab).start()
            else:
                @pl.when(owner != b)
                def _():
                    to_owner(c, 0).start()

                @pl.when(owner == b)
                def _():
                    here = pl.ds((c % subs) * CHUNK, CHUNK)
                    zrecv[0, b, first, here, :] = parts[0][0]
                    zrecv[0, b, second, here, :] = parts[0][1]

    mine = pl.ds(pl.multiple_of(b * rows, rows), rows)
    summed = plane_sum[:, :, mine, :]
    for k in range(1, nb):
        to_peer(k).wait_recv()
        summed = summed + plane_recv[k - 1]
    out_ref[1:3] = summed * (1.0 / 12.0)

    def arrival(kind, source):
        for sub in range(subs):
            pltpu.make_async_remote_copy(
                src_ref=zsend.at[0, 0],
                dst_ref=zrecv.at[kind, source, :, pl.ds(sub * CHUNK, CHUNK), :],
                send_sem=z_send_sem.at[0, 0],
                recv_sem=z_recv_sem.at[kind, source, sub],
                device_id={"band": b, "grid": partner},
            ).wait_recv()

    alike = lax.rem(b, 2) == odd

    @pl.when(alike)
    def _():
        for source in range(nb):
            @pl.when(b != source)
            def _():
                arrival(0, source)
        for source in range(nb):
            arrival(1, source)
        out_ref[0] = (jnp.sum(zrecv[0], 0) + jnp.sum(zrecv[1], 0)) * (1.0 / 12.0)

    @pl.when(jnp.logical_not(alike))
    def _():
        for source in range(nb):
            arrival(0, source)
        out_ref[0] = jnp.sum(zrecv[0], 0) * (1.0 / 12.0)

    for k in range(1, nb):
        to_peer(k).wait_send()
    for c in range(chunks):
        to_mate(c).wait_send()
        to_outer(c).wait_send()
        to_owner(c, 1).wait_send()
        to_owner(c, 2).wait_send()

        @pl.when((c // subs) * 2 + odd != b)
        def _():
            to_owner(c, 0).wait_send()


def solution(mesh):
    nb = mesh.shape["band"]
    ng = mesh.shape["grid"]

    def per_device(orbitals, occupations):
        bands, _, depth, nx, ny = orbitals.shape
        rows = nx // nb
        if depth != 2 or nb % 2 or ng % 2 or ng < 4 or rows % CHUNK:
            raise ValueError("unsupported sizes")
        subs = rows // CHUNK
        chunks = (nb // 2) * subs
        f32, bf16 = jnp.float32, jnp.bfloat16
        dma = pltpu.SemaphoreType.DMA
        return pl.pallas_call(
            functools.partial(kernel, nb, ng),
            out_shape=jax.ShapeDtypeStruct((3, depth, rows, ny), f32),
            in_specs=[
                pl.BlockSpec(memory_space=pltpu.SMEM),
                pl.BlockSpec(memory_space=pl.ANY),
            ],
            out_specs=pl.BlockSpec(memory_space=pltpu.VMEM),
            scratch_shapes=[
                pltpu.VMEM((bands, 2, depth, nx, ny), bf16),
                pltpu.VMEM((chunks, bands, 2, depth, CHUNK, ny), bf16),
                pltpu.VMEM((chunks, bands, 2, depth, CHUNK, ny), bf16),
                pltpu.VMEM((nx, nx), bf16),
                pltpu.VMEM((ny, ny), bf16),
                pltpu.VMEM((2, depth, nx, ny), f32),
                pltpu.VMEM((nb - 1, 2, depth, rows, ny), f32),
                pltpu.VMEM((chunks, 3, depth, CHUNK, ny), f32),
                pltpu.VMEM((2, nb, depth, rows, ny), f32),
                dma,
                dma((chunks,)),
                dma((chunks,)),
                dma((chunks,)),
                dma((chunks,)),
                dma((nb - 1,)),
                dma((nb - 1,)),
                dma((chunks, 3)),
                dma((2, nb, subs)),
                pltpu.SemaphoreType.REGULAR,
            ],
            compiler_params=pltpu.CompilerParams(collective_id=0, has_side_effects=True),
            name="current",
        )(occupations, orbitals)

    return jax.shard_map(
        per_device,
        mesh=mesh,
        in_specs=(P("band", None, "grid", None, None), P("band")),
        out_specs=P(None, "grid", "band", None),
        check_vma=False,
    )
```

```python
import functools

import jax
import jax.numpy as jnp
from jax import lax
from jax.experimental import pallas as pl
from jax.experimental.pallas import tpu as pltpu
from jax.sharding import PartitionSpec as P

CHUNK = 16


def stencil(n, flipped):
    row = lax.broadcasted_iota(jnp.int32, (n, n), 0)
    col = lax.broadcasted_iota(jnp.int32, (n, n), 1)
    d = col - row if flipped else row - col
    value = jnp.zeros((n, n), jnp.float32)
    for step, weight in ((1, 8.0), (-1, -8.0), (2, -1.0), (-2, 1.0)):
        hit = (d == step) | (d == step - n) | (d == step + n)
        value = jnp.where(hit, weight, value)
    return value.astype(jnp.bfloat16)


def kernel(
    nb, ng, occ_ref, orb_ref, out_ref,
    own, mate, outer, mx, my, plane_sum, plane_recv, zsend, zrecv,
    own_sem, mate_send, mate_recv, outer_send, outer_recv,
    plane_send_sem, plane_recv_sem, z_send_sem, z_recv_sem, ready,
):
    bands, _, depth, nx, ny = orb_ref.shape
    b = lax.axis_index("band")
    g = lax.axis_index("grid")
    odd = lax.rem(g, 2)
    turn = 1 - 2 * odd
    partner = g + turn
    ahead = lax.rem(g + 2 * turn + ng, ng)
    behind = lax.rem(g - 2 * turn + ng, ng)
    rows = nx // nb
    subs = rows // CHUNK
    chunks = (nb // 2) * subs

    load = pltpu.make_async_copy(orb_ref, own, own_sem)
    load.start()

    barrier = pltpu.get_barrier_semaphore()
    peers = [lax.rem(b + k, nb) for k in range(1, nb)]
    direct = [(b, partner), (b, ahead), (b, behind)] + [(peer, g) for peer in peers]
    for band, grid in direct:
        pl.semaphore_signal(barrier, inc=1, device_id={"band": band, "grid": grid})
    pl.semaphore_wait(barrier, len(direct))

    def start_of(chunk, parity):
        block = (chunk // subs) * 2 + parity
        return pl.multiple_of(block * rows + (chunk % subs) * CHUNK, CHUNK)

    def to_mate(c):
        return pltpu.make_async_remote_copy(
            src_ref=orb_ref.at[:, :, :, pl.ds(start_of(c, 1 - odd), CHUNK), :],
            dst_ref=mate.at[c],
            send_sem=mate_send.at[c],
            recv_sem=mate_recv.at[c],
            device_id={"band": b, "grid": partner},
        )

    def to_outer(c):
        return pltpu.make_async_remote_copy(
            src_ref=orb_ref.at[:, :, :, pl.ds(start_of(c, odd), CHUNK), :],
            dst_ref=outer.at[c],
            send_sem=outer_send.at[c],
            recv_sem=outer_recv.at[c],
            device_id={"band": b, "grid": behind},
        )

    for c in range(chunks):
        to_mate(c).start()
        to_outer(c).start()
    for peer in peers:
        pl.semaphore_signal(ready, inc=1, device_id={"band": peer, "grid": g})

    mx[...] = stencil(nx, True)
    my[...] = stencil(ny, False)
    plane_sum[...] = jnp.zeros_like(plane_sum)
    load.wait()

    def lateral(n, carry):
        w = occ_ref[n]
        for s in range(depth):
            re = own[n, 0, s]
            im = own[n, 1, s]
            tx = jnp.dot(mx[...], jnp.concatenate([re, im], 1), preferred_element_type=jnp.float32)
            ty = jnp.dot(jnp.concatenate([re, im], 0), my[...], preferred_element_type=jnp.float32)
            wre = re.astype(jnp.float32) * w
            wim = im.astype(jnp.float32) * w
            plane_sum[0, s] += wre * tx[:, ny:] - wim * tx[:, :ny]
            plane_sum[1, s] += wre * ty[nx:] - wim * ty[:nx]
        return carry

    lax.fori_loop(0, bands, lateral, 0)

    def to_peer(k):
        peer = lax.rem(b + k, nb)
        return pltpu.make_async_remote_copy(
            src_ref=plane_sum.at[:, :, pl.ds(pl.multiple_of(peer * rows, rows), rows), :],
            dst_ref=plane_recv.at[k - 1],
            send_sem=plane_send_sem.at[k - 1],
            recv_sem=plane_recv_sem.at[k - 1],
            device_id={"band": peer, "grid": g},
        )

    for k in range(1, nb):
        to_peer(k).start()

    pl.semaphore_wait(ready, nb - 1)
    sign = turn.astype(jnp.float32)
    first = odd
    second = 1 - odd

    def to_owner(c, slab):
        at = (g, partner, ahead)[slab]
        sub = c % subs
        return pltpu.make_async_remote_copy(
            src_ref=zsend.at[c, slab],
            dst_ref=zrecv.at[slab // 2, b, :, pl.ds(sub * CHUNK, CHUNK), :],
            send_sem=z_send_sem.at[c, slab],
            recv_sem=z_recv_sem.at[slab // 2, b, sub],
            device_id={"band": (c // subs) * 2 + odd, "grid": at},
        )

    for c in range(chunks):
        if c == chunks - 1:
            mine = pl.ds(pl.multiple_of(b * rows, rows), rows)
            summed = plane_sum[:, :, mine, :]
            for k in range(1, nb):
                to_peer(k).wait_recv()
                summed = summed + plane_recv[k - 1]
            out_ref[1:3] = summed * (1.0 / 12.0)
        start = start_of(c, odd)
        to_mate(c).wait_recv()
        to_outer(c).wait_recv()

        def depthwise(n, sums):
            w = occ_ref[n] * sign
            fields = []
            for p in (first, second):
                fields.append(tuple(own[n, q, p, pl.ds(start, CHUNK), :].astype(jnp.float32) for q in (0, 1)))
            for held in (mate, outer):
                for p in (first, second):
                    fields.append(tuple(held[c, n, q, p].astype(jnp.float32) for q in (0, 1)))
            scaled = [(re * w, im * w) for re, im in fields[:4]]
            pairs = ((0, 1), (1, 2), (2, 3), (3, 4), (0, 2), (1, 3), (2, 4), (3, 5))
            return tuple(
                total + (scaled[i][0] * fields[j][1] - scaled[i][1] * fields[j][0])
                for total, (i, j) in zip(sums, pairs)
            )

        zero = jnp.zeros((CHUNK, ny), jnp.float32)
        n01, n12, n23, n34, f02, f13, f24, f35 = lax.fori_loop(0, bands, depthwise, (zero,) * 8)
        parts = (
            (8.0 * n01 - f02, 8.0 * (n01 + n12) - f13),
            (8.0 * (n12 + n23) - f02 - f24, 8.0 * (n23 + n34) - f13 - f35),
            (8.0 * n34 - f24, -f35),
        )
        owner = (c // subs) * 2 + odd
        for slab in (1, 2, 0):
            zsend[c, slab, first] = parts[slab][0]
            zsend[c, slab, second] = parts[slab][1]
            if slab:
                to_owner(c, slab).start()
            else:
                @pl.when(owner != b)
                def _():
                    to_owner(c, 0).start()

                @pl.when(owner == b)
                def _():
                    here = pl.ds((c % subs) * CHUNK, CHUNK)
                    zrecv[0, b, first, here, :] = parts[0][0]
                    zrecv[0, b, second, here, :] = parts[0][1]

    def arrival(kind, source):
        for sub in range(subs):
            pltpu.make_async_remote_copy(
                src_ref=zsend.at[0, 0],
                dst_ref=zrecv.at[kind, source, :, pl.ds(sub * CHUNK, CHUNK), :],
                send_sem=z_send_sem.at[0, 0],
                recv_sem=z_recv_sem.at[kind, source, sub],
                device_id={"band": b, "grid": partner},
            ).wait_recv()

    alike = lax.rem(b, 2) == odd

    @pl.when(alike)
    def _():
        for source in range(nb):
            @pl.when(b != source)
            def _():
                arrival(0, source)
        for source in range(nb):
            arrival(1, source)
        out_ref[0] = (jnp.sum(zrecv[0], 0) + jnp.sum(zrecv[1], 0)) * (1.0 / 12.0)

    @pl.when(jnp.logical_not(alike))
    def _():
        for source in range(nb):
            arrival(0, source)
        out_ref[0] = jnp.sum(zrecv[0], 0) * (1.0 / 12.0)

    for k in range(1, nb):
        to_peer(k).wait_send()
    for c in range(chunks):
        to_mate(c).wait_send()
        to_outer(c).wait_send()
        to_owner(c, 1).wait_send()
        to_owner(c, 2).wait_send()

        @pl.when((c // subs) * 2 + odd != b)
        def _():
            to_owner(c, 0).wait_send()


def solution(mesh):
    nb = mesh.shape["band"]
    ng = mesh.shape["grid"]

    def per_device(orbitals, occupations):
        bands, _, depth, nx, ny = orbitals.shape
        rows = nx // nb
        if depth != 2 or nb % 2 or ng % 2 or ng < 4 or rows % CHUNK:
            raise ValueError("unsupported sizes")
        subs = rows // CHUNK
        chunks = (nb // 2) * subs
        f32, bf16 = jnp.float32, jnp.bfloat16
        dma = pltpu.SemaphoreType.DMA
        return pl.pallas_call(
            functools.partial(kernel, nb, ng),
            out_shape=jax.ShapeDtypeStruct((3, depth, rows, ny), f32),
            in_specs=[
                pl.BlockSpec(memory_space=pltpu.SMEM),
                pl.BlockSpec(memory_space=pl.ANY),
            ],
            out_specs=pl.BlockSpec(memory_space=pltpu.VMEM),
            scratch_shapes=[
                pltpu.VMEM((bands, 2, depth, nx, ny), bf16),
                pltpu.VMEM((chunks, bands, 2, depth, CHUNK, ny), bf16),
                pltpu.VMEM((chunks, bands, 2, depth, CHUNK, ny), bf16),
                pltpu.VMEM((nx, nx), bf16),
                pltpu.VMEM((ny, ny), bf16),
                pltpu.VMEM((2, depth, nx, ny), f32),
                pltpu.VMEM((nb - 1, 2, depth, rows, ny), f32),
                pltpu.VMEM((chunks, 3, depth, CHUNK, ny), f32),
                pltpu.VMEM((2, nb, depth, rows, ny), f32),
                dma,
                dma((chunks,)),
                dma((chunks,)),
                dma((chunks,)),
                dma((chunks,)),
                dma((nb - 1,)),
                dma((nb - 1,)),
                dma((chunks, 3)),
                dma((2, nb, subs)),
                pltpu.SemaphoreType.REGULAR,
            ],
            compiler_params=pltpu.CompilerParams(collective_id=0, has_side_effects=True, vmem_limit_bytes=55000 * 1024),
            name="current",
        )(occupations, orbitals)

    return jax.shard_map(
        per_device,
        mesh=mesh,
        in_specs=(P("band", None, "grid", None, None), P("band")),
        out_specs=P(None, "grid", "band", None),
        check_vma=False,
    )
```

```python
import functools

import jax
import jax.numpy as jnp
from jax import lax
from jax.experimental import pallas as pl
from jax.experimental.pallas import tpu as pltpu
from jax.sharding import PartitionSpec as P

CHUNK = 16


def stencil(n, flipped):
    row = lax.broadcasted_iota(jnp.int32, (n, n), 0)
    col = lax.broadcasted_iota(jnp.int32, (n, n), 1)
    d = col - row if flipped else row - col
    value = jnp.zeros((n, n), jnp.float32)
    for step, weight in ((1, 8.0), (-1, -8.0), (2, -1.0), (-2, 1.0)):
        hit = (d == step) | (d == step - n) | (d == step + n)
        value = jnp.where(hit, weight, value)
    return value.astype(jnp.bfloat16)


def kernel(
    nb, ng, occ_ref, orb_ref, out_ref,
    own, mate, outer, mx, my, plane_sum, plane_recv, zsend, zrecv,
    own_sem, mate_send, mate_recv, outer_send, outer_recv,
    plane_send_sem, plane_recv_sem, z_send_sem, z_recv_sem, ready,
):
    bands, _, depth, nx, ny = orb_ref.shape
    b = lax.axis_index("band")
    g = lax.axis_index("grid")
    odd = lax.rem(g, 2)
    turn = 1 - 2 * odd
    partner = g + turn
    ahead = lax.rem(g + 2 * turn + ng, ng)
    behind = lax.rem(g - 2 * turn + ng, ng)
    rows = nx // nb
    subs = rows // CHUNK
    chunks = (nb // 2) * subs

    load = pltpu.make_async_copy(orb_ref, own, own_sem)
    load.start()

    barrier = pltpu.get_barrier_semaphore()
    peers = [lax.rem(b + k, nb) for k in range(1, nb)]
    direct = [(b, partner), (b, ahead), (b, behind)] + [(peer, g) for peer in peers]
    for band, grid in direct:
        pl.semaphore_signal(barrier, inc=1, device_id={"band": band, "grid": grid})
    pl.semaphore_wait(barrier, len(direct))

    def start_of(chunk, parity):
        block = (chunk // subs) * 2 + parity
        return pl.multiple_of(block * rows + (chunk % subs) * CHUNK, CHUNK)

    def to_mate(c):
        return pltpu.make_async_remote_copy(
            src_ref=orb_ref.at[:, :, :, pl.ds(start_of(c, 1 - odd), CHUNK), :],
            dst_ref=mate.at[c],
            send_sem=mate_send.at[c],
            recv_sem=mate_recv.at[c],
            device_id={"band": b, "grid": partner},
        )

    def to_outer(c):
        return pltpu.make_async_remote_copy(
            src_ref=orb_ref.at[:, :, :, pl.ds(start_of(c, odd), CHUNK), :],
            dst_ref=outer.at[c],
            send_sem=outer_send.at[c],
            recv_sem=outer_recv.at[c],
            device_id={"band": b, "grid": behind},
        )

    for c in range(chunks):
        to_mate(c).start()
        to_outer(c).start()
    for peer in peers:
        pl.semaphore_signal(ready, inc=1, device_id={"band": peer, "grid": g})

    mx[...] = stencil(nx, True)
    my[...] = stencil(ny, False)
    plane_sum[...] = jnp.zeros_like(plane_sum)
    load.wait()

    def lateral(n, carry):
        w = occ_ref[n]
        for s in range(depth):
            re = own[n, 0, s]
            im = own[n, 1, s]
            tx = jnp.dot(mx[...], jnp.concatenate([re, im], 1), preferred_element_type=jnp.float32)
            ty = jnp.dot(jnp.concatenate([re, im], 0), my[...], preferred_element_type=jnp.float32)
            wre = re.astype(jnp.float32) * w
            wim = im.astype(jnp.float32) * w
            plane_sum[0, s] += wre * tx[:, ny:] - wim * tx[:, :ny]
            plane_sum[1, s] += wre * ty[nx:] - wim * ty[:nx]
        return carry

    lax.fori_loop(0, bands, lateral, 0)

    def to_peer(k):
        peer = lax.rem(b + k, nb)
        return pltpu.make_async_remote_copy(
            src_ref=plane_sum.at[:, :, pl.ds(pl.multiple_of(peer * rows, rows), rows), :],
            dst_ref=plane_recv.at[k - 1],
            send_sem=plane_send_sem.at[k - 1],
            recv_sem=plane_recv_sem.at[k - 1],
            device_id={"band": peer, "grid": g},
        )

    for k in range(1, nb):
        to_peer(k).start()

    pl.semaphore_wait(ready, nb - 1)
    sign = turn.astype(jnp.float32)
    first = odd
    second = 1 - odd

    def to_owner(c, slab):
        at = (g, partner, ahead)[slab]
        sub = c % subs
        return pltpu.make_async_remote_copy(
            src_ref=zsend.at[c, slab],
            dst_ref=zrecv.at[slab // 2, b, :, pl.ds(sub * CHUNK, CHUNK), :],
            send_sem=z_send_sem.at[c, slab],
            recv_sem=z_recv_sem.at[slab // 2, b, sub],
            device_id={"band": (c // subs) * 2 + odd, "grid": at},
        )

    for c in range(chunks):
        if c == chunks - 1:
            mine = pl.ds(pl.multiple_of(b * rows, rows), rows)
            summed = plane_sum[:, :, mine, :]
            for k in range(1, nb):
                to_peer(k).wait_recv()
                summed = summed + plane_recv[k - 1]
            out_ref[1:3] = summed * (1.0 / 12.0)
        start = start_of(c, odd)
        to_mate(c).wait_recv()
        to_outer(c).wait_recv()

        def depthwise(n, sums):
            w = occ_ref[n] * sign
            fields = []
            for p in (first, second):
                fields.append(tuple(own[n, q, p, pl.ds(start, CHUNK), :].astype(jnp.float32) for q in (0, 1)))
            for held in (mate, outer):
                for p in (first, second):
                    fields.append(tuple(held[c, n, q, p].astype(jnp.float32) for q in (0, 1)))
            scaled = [(re * w, im * w) for re, im in fields[:4]]
            pairs = ((0, 1), (1, 2), (2, 3), (3, 4), (0, 2), (1, 3), (2, 4), (3, 5))
            return tuple(
                total + (scaled[i][0] * fields[j][1] - scaled[i][1] * fields[j][0])
                for total, (i, j) in zip(sums, pairs)
            )

        zero = jnp.zeros((CHUNK, ny), jnp.float32)
        n01, n12, n23, n34, f02, f13, f24, f35 = lax.fori_loop(0, bands, depthwise, (zero,) * 8, unroll=4)
        parts = (
            (8.0 * n01 - f02, 8.0 * (n01 + n12) - f13),
            (8.0 * (n12 + n23) - f02 - f24, 8.0 * (n23 + n34) - f13 - f35),
            (8.0 * n34 - f24, -f35),
        )
        owner = (c // subs) * 2 + odd
        for slab in (1, 2, 0):
            zsend[c, slab, first] = parts[slab][0]
            zsend[c, slab, second] = parts[slab][1]
            if slab:
                to_owner(c, slab).start()
            else:
                @pl.when(owner != b)
                def _():
                    to_owner(c, 0).start()

                @pl.when(owner == b)
                def _():
                    here = pl.ds((c % subs) * CHUNK, CHUNK)
                    zrecv[0, b, first, here, :] = parts[0][0]
                    zrecv[0, b, second, here, :] = parts[0][1]

    def arrival(kind, source):
        for sub in range(subs):
            pltpu.make_async_remote_copy(
                src_ref=zsend.at[0, 0],
                dst_ref=zrecv.at[kind, source, :, pl.ds(sub * CHUNK, CHUNK), :],
                send_sem=z_send_sem.at[0, 0],
                recv_sem=z_recv_sem.at[kind, source, sub],
                device_id={"band": b, "grid": partner},
            ).wait_recv()

    alike = lax.rem(b, 2) == odd

    @pl.when(alike)
    def _():
        for source in range(nb):
            @pl.when(b != source)
            def _():
                arrival(0, source)
        for source in range(nb):
            arrival(1, source)
        out_ref[0] = (jnp.sum(zrecv[0], 0) + jnp.sum(zrecv[1], 0)) * (1.0 / 12.0)

    @pl.when(jnp.logical_not(alike))
    def _():
        for source in range(nb):
            arrival(0, source)
        out_ref[0] = jnp.sum(zrecv[0], 0) * (1.0 / 12.0)

    for k in range(1, nb):
        to_peer(k).wait_send()
    for c in range(chunks):
        to_mate(c).wait_send()
        to_outer(c).wait_send()
        to_owner(c, 1).wait_send()
        to_owner(c, 2).wait_send()

        @pl.when((c // subs) * 2 + odd != b)
        def _():
            to_owner(c, 0).wait_send()


def solution(mesh):
    nb = mesh.shape["band"]
    ng = mesh.shape["grid"]

    def per_device(orbitals, occupations):
        bands, _, depth, nx, ny = orbitals.shape
        rows = nx // nb
        if depth != 2 or nb % 2 or ng % 2 or ng < 4 or rows % CHUNK:
            raise ValueError("unsupported sizes")
        subs = rows // CHUNK
        chunks = (nb // 2) * subs
        f32, bf16 = jnp.float32, jnp.bfloat16
        dma = pltpu.SemaphoreType.DMA
        return pl.pallas_call(
            functools.partial(kernel, nb, ng),
            out_shape=jax.ShapeDtypeStruct((3, depth, rows, ny), f32),
            in_specs=[
                pl.BlockSpec(memory_space=pltpu.SMEM),
                pl.BlockSpec(memory_space=pl.ANY),
            ],
            out_specs=pl.BlockSpec(memory_space=pltpu.VMEM),
            scratch_shapes=[
                pltpu.VMEM((bands, 2, depth, nx, ny), bf16),
                pltpu.VMEM((chunks, bands, 2, depth, CHUNK, ny), bf16),
                pltpu.VMEM((chunks, bands, 2, depth, CHUNK, ny), bf16),
                pltpu.VMEM((nx, nx), bf16),
                pltpu.VMEM((ny, ny), bf16),
                pltpu.VMEM((2, depth, nx, ny), f32),
                pltpu.VMEM((nb - 1, 2, depth, rows, ny), f32),
                pltpu.VMEM((chunks, 3, depth, CHUNK, ny), f32),
                pltpu.VMEM((2, nb, depth, rows, ny), f32),
                dma,
                dma((chunks,)),
                dma((chunks,)),
                dma((chunks,)),
                dma((chunks,)),
                dma((nb - 1,)),
                dma((nb - 1,)),
                dma((chunks, 3)),
                dma((2, nb, subs)),
                pltpu.SemaphoreType.REGULAR,
            ],
            compiler_params=pltpu.CompilerParams(collective_id=0, has_side_effects=True, vmem_limit_bytes=55000 * 1024),
            name="current",
        )(occupations, orbitals)

    return jax.shard_map(
        per_device,
        mesh=mesh,
        in_specs=(P("band", None, "grid", None, None), P("band")),
        out_specs=P(None, "grid", "band", None),
        check_vma=False,
    )
```
